32 devices in a mesh: row: 4 (over x, core), col: 8 (over z, y).
Axes of the slice: x: 2, y: 2, z: 4, core: 2. Of those that a mesh axis runs over, the one named last changes fastest.
Arguments:
- points: float32 [16, 8192], P(None, ('row', 'col')), may hold values from -6 to 6
- lengthscale: float32 [16], replicated, may hold values from 2 to 8
- signal: float32 [1], replicated, may hold values from 0.5 to 2
- noise: float32 [1], replicated, may hold values from 0.05 to 0.5
- targets: float32 [8192], P(('row', 'col')), may hold values from -12 to 12
- probe_bits: int32 [31, 8192], P(None, ('row', 'col')), may hold values from 0 to 1
Outputs:
- solution: float32 [32, 8192], P(None, ('row', 'col'))
- residual: float32 [32, 8192], P(None, ('row', 'col'))
The draws below stay inside these ranges and needn't reach their ends.
All inputs are finite; a program needn't handle non-finite values.
Results may differ from the reference program's by a relative error of at most 0.0013.
Values sent between devices are 32-bit elements; how exact they have to be, the bound alone decides.
No kernel may reach another device: no remote copies, remote signals or barrier semaphores. Data moves between devices by JAX's collectives and lax.ppermute only.
A program may use at most 128 MiB of HBM per device.

```python
import math
import jax
import jax.numpy as jnp
from jax import lax

DIM = 16
PROBES = 31
ITERS = 3
N = 8192


def draw_targets(key, part):
    ramp = 1.0 + 2.0 * jnp.arange(N, dtype=jnp.float32) / N
    values = jnp.clip(jax.random.normal(key, (N,), jnp.float32), -4.0, 4.0)
    return values * ramp


def with_ends(array, stream_key, least, high):
    index_at = [jax.random.randint(jax.random.fold_in(stream_key, axis), (), 0, length) for axis, length in enumerate(array.shape)]
    longest = array.shape.index(max(array.shape))
    next_to = index_at[:longest] + [(index_at[longest] + 1) % array.shape[longest]] + index_at[longest + 1:]
    return array.at[tuple(index_at)].set(least).at[tuple(next_to)].set(high)


def level_of(stream_key, extent, split, low, high):
    def one(position, parts):
        draws = jax.random.uniform(jax.random.fold_in(jax.random.fold_in(stream_key, 6), position), (parts,), jnp.float32, low / len(split), high / len(split))
        return jnp.repeat(jnp.exp(draws), extent[position] // parts).reshape((-1,) + (1,) * (len(extent) - position - 1))

    factor_of = one(*split[0])
    for cut in split[1:]:
        factor_of = factor_of * one(*cut)
    return factor_of


def gaussian(stream_key, dims, spread, most, cuts=(), kind=jnp.bfloat16):
    values = jax.random.normal(stream_key, dims, jnp.float32) * spread
    if len(cuts) > 0:
        values = level_of(stream_key, dims, cuts, -0.22, 0.18) * values
    return jnp.clip(values, min=-most, max=most).astype(kind)


def setup_inputs(seed: int = 0) -> dict:
    keys = jax.random.split(jax.random.key(seed), 7)
    return {
        "points": gaussian(keys[0], (DIM, N), 1.0, 6.0, ((1, 32),), jnp.float32),
        "lengthscale": jnp.clip(jnp.exp(jax.random.uniform(keys[1], (DIM,), jnp.float32, math.log(2.0), math.log(8.0))), 2.0, 8.0),
        "signal": jnp.clip(jnp.exp(jax.random.uniform(keys[2], (1,), jnp.float32, math.log(0.5), math.log(2.0))), 0.5, 2.0),
        "noise": jnp.clip(jnp.exp(jax.random.uniform(keys[3], (1,), jnp.float32, math.log(0.05), math.log(0.5))), 0.05, 0.5),
        "targets": draw_targets(jax.random.fold_in(keys[6], 71), 0),
        "probe_bits": with_ends(jax.random.randint(keys[5], (PROBES, N), 0, 2), jax.random.fold_in(keys[5], 1), 0, 1).astype(jnp.int32),
    }


ROOT_FIVE = 5.0 ** 0.5

def matern_tile(row_scaled, col_scaled, signal_value):
    row_sq = lax.optimization_barrier(jnp.sum(row_scaled * row_scaled, axis=0))
    col_sq = lax.optimization_barrier(jnp.sum(col_scaled * col_scaled, axis=0))
    cross_term = lax.dot_general(row_scaled, col_scaled, (((0,), (0,)), ((), ())), precision=lax.Precision.HIGHEST, preferred_element_type=jnp.float32)
    dist_sq = jnp.maximum(row_sq[:, None] + col_sq[None, :] - 2.0 * cross_term, 0.0)
    radius = jnp.sqrt(dist_sq)
    return signal_value * (1.0 + ROOT_FIVE * radius + 5.0 / 3.0 * dist_sq) * jnp.exp(-ROOT_FIVE * radius)

def reference(points, lengthscale, signal, noise, targets, probe_bits):
    scaled = points / lengthscale[:, None]
    signs = 2.0 * probe_bits.astype(jnp.float32) - 1.0
    right_side = jnp.concatenate([targets[None, :], signs], axis=0)
    signal_value = signal[0]
    noise_value = noise[0]
    block_rows = min(2048, N)
    stacked = scaled.reshape(DIM, N // block_rows, block_rows).transpose(1, 0, 2)

    def operator(vectors):

        def one_block(row_block):
            kernel_tile = matern_tile(row_block, scaled, signal_value)
            return lax.dot_general(vectors, kernel_tile, (((1,), (1,)), ((), ())), precision=lax.Precision.HIGHEST, preferred_element_type=jnp.float32)
        pieces = lax.map(one_block, stacked)
        return pieces.transpose(1, 0, 2).reshape(vectors.shape[0], N) + noise_value * vectors
    solution = jnp.zeros_like(right_side)
    residual = right_side
    direction = right_side
    norm_now = lax.optimization_barrier(jnp.sum(residual * residual, axis=1))
    for step in range(ITERS):
        image = operator(direction)
        alpha = norm_now / lax.optimization_barrier(jnp.sum(direction * image, axis=1))
        solution = solution + alpha[:, None] * direction
        residual = residual - alpha[:, None] * image
        if step + 1 < ITERS:
            norm_next = lax.optimization_barrier(jnp.sum(residual * residual, axis=1))
            direction = residual + (norm_next / norm_now)[:, None] * direction
            norm_now = norm_next
    return (solution, residual)
```

```python
import functools

import jax
import jax.numpy as jnp
from jax import lax
from jax.experimental import pallas as pl
from jax.experimental.pallas import tpu as pltpu
from jax.sharding import PartitionSpec as P

ITERS = 3
AXES = ("row", "col")
ROOT_FIVE = 5.0**0.5
LOG2_E = 1.4426950408889634


def bits_of(n):
    return [1 << k for k in range(n.bit_length() - 1)]


def phases_of(rows, cols):
    col_bits = bits_of(cols)
    row_bits = [b * cols for b in bits_of(rows)]
    first = col_bits[-2:]
    rest = col_bits[:-2] + row_bits[1:]
    groups = [first] + [rest[k : k + 2] for k in range(0, len(rest), 2)]
    return [g for g in groups if g], row_bits[0]


def masks_of(bits):
    masks = [0]
    for b in bits:
        masks += [m | b for m in masks]
    return masks[1:]


def gather(block, mesh_shape):
    rows, cols = mesh_shape
    count = rows * cols

    def swap(value, mask):
        return lax.ppermute(value, AXES, [(d, d ^ mask) for d in range(count)])

    groups, core = phases_of(rows, cols)
    held = block[None]
    for number, bits in enumerate(groups):
        parts = [held] + [swap(held, m) for m in masks_of(bits)]
        if number + 1 < len(groups):
            held = jnp.concatenate(parts, axis=0)
    return parts + [swap(p, core) for p in parts]


def split_two(value):
    high = value.astype(jnp.bfloat16)
    low = (value - high.astype(jnp.float32)).astype(jnp.bfloat16)
    return high, low


def split_three(value):
    high = value.astype(jnp.bfloat16).astype(jnp.float32)
    rest = value - high
    middle = rest.astype(jnp.bfloat16).astype(jnp.float32)
    return high, middle, rest - middle


def features(points, own):
    high, middle, low = split_three(points)
    norm = jnp.sum(points * points, axis=0, keepdims=True)
    ones = jnp.ones_like(norm)
    zeros = jnp.zeros((2, norm.shape[1]), jnp.float32)
    norms = list(split_three(norm))
    if own:
        stack = [-2.0 * q for q in (high, high, middle, middle, high, low)]
        tail = [ones, ones, ones] + norms + [zeros]
    else:
        stack = [high, middle, high, middle, low, high]
        tail = norms + [ones, ones, ones, zeros]
    pad = jnp.zeros((8, norm.shape[1]), jnp.float32)
    return jnp.concatenate(stack + [jnp.concatenate(tail, axis=0), pad], axis=0).astype(jnp.bfloat16)


def times(vector, high_ref, low_ref, block):
    width = vector.shape[1]
    rows = pl.ds(pl.multiple_of(block * width, width), width)
    v_high, v_low = split_two(vector)
    both = jnp.dot(
        jnp.concatenate([v_high, v_low], axis=0), high_ref[rows, :], preferred_element_type=jnp.float32
    )
    count = vector.shape[0]
    return (both[:count] + both[count:]) + jnp.dot(v_high, low_ref[rows, :], preferred_element_type=jnp.float32)


def copy_pieces(refs, out_ref, start=0):
    at = 0
    for ref in refs:
        m = ref.shape[0]
        for k in range(m):
            out_ref[at + k] = ref[k, start:, :]
        at += m


def build_kernel(pieces, dim, *refs):
    ins, (scale_ref, high_ref, low_ref, vec_ref, image_ref, points_ref) = refs[:pieces], refs[pieces:]
    at = 0
    for ref in ins:
        for k in range(ref.shape[0]):
            points_ref[at + k] = ref[k, :dim, :]
            vec_ref[at + k] = ref[k, dim:, :]
        at += ref.shape[0]
    blocks = at
    own = features(points_ref[0], True)
    width = own.shape[1]

    def one(block, total):
        rows = pl.ds(pl.multiple_of(block * width, width), width)
        dist = lax.dot_general(
            features(points_ref[block], False),
            own,
            (((0,), (0,)), ((), ())),
            preferred_element_type=jnp.float32,
        )
        dist = jnp.maximum(dist, 1e-30)
        radius = dist * lax.rsqrt(dist)
        tile = ((1.0 + dist * (1.0 / 3.0)) + radius) * jnp.exp2(radius * (-LOG2_E))
        high, low = split_two(tile)
        high_ref[rows, :] = high
        low_ref[rows, :] = low
        return total + times(vec_ref[block], high_ref, low_ref, block)

    total = lax.fori_loop(0, blocks, one, jnp.zeros(image_ref.shape, jnp.float32))
    image_ref[...] = scale_ref[0] * total + scale_ref[1] * vec_ref[0]


def total_of(left_ref, right_ref):
    blocks, count, width = left_ref.shape

    def one(block, total):
        return total + left_ref[block] * right_ref[block]

    total = lax.fori_loop(0, blocks, one, jnp.zeros((count, width), jnp.float32))
    return jnp.sum(total, axis=1, keepdims=True)


def step_kernel(pieces, first, last, *refs):
    ins, refs = refs[:pieces], refs[pieces:]
    scale_ref, high_ref, low_ref, res_ref, dir_ref, norm_ref, sol_ref = refs[:7]
    new_res_ref, new_dir_ref, new_norm_ref, new_sol_ref, image_ref = refs[7:12]
    img_ref = refs[12]
    copy_pieces(ins, img_ref)
    blocks, count, width = img_ref.shape
    norm = total_of(res_ref, res_ref) if first else norm_ref[...]
    alpha = norm / total_of(dir_ref, img_ref)
    new_sol = alpha * dir_ref[0]
    new_sol_ref[...] = new_sol if first else sol_ref[...] + new_sol

    def update(block, total):
        res = res_ref[block] - alpha * img_ref[block]
        new_res_ref[block] = res
        return total + res * res

    total = lax.fori_loop(0, blocks, update, jnp.zeros((count, width), jnp.float32))
    new_norm = jnp.sum(total, axis=1, keepdims=True)
    new_norm_ref[...] = new_norm
    beta = new_norm / norm

    def one(block, total):
        direction = new_res_ref[block] + beta * dir_ref[block]
        new_dir_ref[block] = direction
        return total + times(direction, high_ref, low_ref, block)

    total = lax.fori_loop(0, blocks, one, jnp.zeros((count, width), jnp.float32))
    image_ref[...] = scale_ref[0] * total + scale_ref[1] * new_dir_ref[0]


VMEM = pl.BlockSpec(memory_space=pltpu.VMEM)
SMEM = pl.BlockSpec(memory_space=pltpu.SMEM)


def body(mesh_shape, points, lengthscale, signal, noise, targets, probe_bits):
    devices = mesh_shape[0] * mesh_shape[1]
    dim, width = points.shape
    count = probe_bits.shape[0] + 1
    f32 = jnp.float32
    vectors = jax.ShapeDtypeStruct((devices, count, width), f32)
    column = jax.ShapeDtypeStruct((count, 1), f32)
    local = jax.ShapeDtypeStruct((count, width), f32)
    matrix = jax.ShapeDtypeStruct((devices * width, width), jnp.bfloat16)

    scaled = points / lengthscale[:, None] * ROOT_FIVE
    signs = 2.0 * probe_bits.astype(f32) - 1.0
    payload = jnp.concatenate([scaled, targets[None, :], signs], axis=0)
    scale = jnp.concatenate([signal, noise])
    pieces = gather(payload, mesh_shape)
    flops = 2 * devices * width * width
    high, low, right_side, image = pl.pallas_call(
        functools.partial(build_kernel, len(pieces), dim),
        out_shape=(matrix, matrix, vectors, local),
        in_specs=[VMEM] * len(pieces) + [SMEM],
        out_specs=(VMEM,) * 4,
        scratch_shapes=[pltpu.VMEM((devices, dim, width), f32)],
        cost_estimate=pl.CostEstimate(flops=flops * 300, bytes_accessed=4 * devices * width * width, transcendentals=0),
    )(*pieces, scale)

    residual = direction = right_side
    norm = jnp.zeros((count, 1), f32)
    so_far = jnp.zeros((count, width), f32)
    for number in range(ITERS - 1):
        pieces = gather(image, mesh_shape)
        residual, direction, norm, so_far, image = pl.pallas_call(
            functools.partial(step_kernel, len(pieces), number == 0, number == ITERS - 2),
            out_shape=(vectors, vectors, column, local, local),
            in_specs=[VMEM] * len(pieces) + [SMEM] + [VMEM] * 6,
            out_specs=(VMEM,) * 5,
            scratch_shapes=[pltpu.VMEM((devices, count, width), f32)],
            cost_estimate=pl.CostEstimate(flops=flops * 100, bytes_accessed=4 * devices * width * width, transcendentals=0),
        )(*pieces, scale, high, low, residual, direction, norm, so_far)
    residual, direction = residual[0], direction[0]
    share = jnp.sum(direction * image, axis=1)
    shares = lax.all_to_all(jnp.broadcast_to(share[None], (devices, count)), AXES, 0, 0)
    alpha = norm / jnp.sum(shares, axis=0)[:, None]
    return (so_far + alpha * direction, residual - alpha * image)


def solution(mesh):
    shape = (mesh.shape["row"], mesh.shape["col"])
    return jax.shard_map(
        functools.partial(body, shape),
        mesh=mesh,
        in_specs=(
            P(None, AXES),
            P(),
            P(),
            P(),
            P(AXES),
            P(None, AXES),
        ),
        out_specs=(P(None, AXES), P(None, AXES)),
        check_vma=False,
    )
```

```python
import functools
import math

import jax
import jax.numpy as jnp
from jax import lax
from jax.experimental import pallas as pl
from jax.experimental.pallas import tpu as pltpu
from jax.sharding import PartitionSpec as P

ITERS = 3
AXES = ("row", "col")
ROOT_FIVE = 5.0**0.5
FEATURES = 112
LOG2_E = 1.4426950408889634


def bits_of(n):
    return [1 << k for k in range(n.bit_length() - 1)]


def phases_of(rows, cols):
    col_bits = bits_of(cols)
    row_bits = [b * cols for b in bits_of(rows)]
    first = col_bits[-2:]
    rest = col_bits[:-2] + row_bits[1:]
    groups = [first] + [rest[k : k + 2] for k in range(0, len(rest), 2)]
    return [g for g in groups if g], row_bits[0]


def masks_of(bits):
    masks = [0]
    for b in bits:
        masks += [m | b for m in masks]
    return masks[1:]


def gather(block, mesh_shape):
    rows, cols = mesh_shape
    count = rows * cols

    def swap(value, mask):
        return lax.ppermute(value, AXES, [(d, d ^ mask) for d in range(count)])

    groups, core = phases_of(rows, cols)
    held = block[None]
    for number, bits in enumerate(groups):
        parts = [held] + [swap(held, m) for m in masks_of(bits)]
        if number + 1 < len(groups):
            held = jnp.concatenate(parts, axis=0)
    return parts + [swap(p, core) for p in parts]


def split_two(value):
    high = value.astype(jnp.bfloat16)
    low = (value - high.astype(jnp.float32)).astype(jnp.bfloat16)
    return high, low


def split_three(value):
    high = value.astype(jnp.bfloat16).astype(jnp.float32)
    rest = value - high
    middle = rest.astype(jnp.bfloat16).astype(jnp.float32)
    return high, middle, rest - middle


def features(points, own):
    high, middle, low = split_three(points)
    norm = jnp.sum(points * points, axis=0, keepdims=True)
    ones = jnp.ones_like(norm)
    zeros = jnp.zeros((2, norm.shape[1]), jnp.float32)
    norms = list(split_three(norm))
    if own:
        stack = [-2.0 * q for q in (high, high, middle, middle, high, low)]
        tail = [ones, ones, ones] + norms + [zeros]
    else:
        stack = [high, middle, high, middle, low, high]
        tail = norms + [ones, ones, ones, zeros]
    pad = jnp.zeros((8, norm.shape[1]), jnp.float32)
    return jnp.concatenate(stack + [jnp.concatenate(tail, axis=0), pad], axis=0).astype(jnp.bfloat16)


def columns(block, width):
    return pl.ds(block * width, width)


def payload_kernel(points_ref, length_ref, targets_ref, bits_ref, out_ref):
    dim, width = points_ref.shape
    rows = [points_ref[k : k + 1, :] / jnp.full((1, width), length_ref[k], jnp.float32) for k in range(dim)]
    out_ref[:dim, :] = jnp.concatenate(rows, axis=0) * ROOT_FIVE
    out_ref[dim : dim + 1, :] = targets_ref[...][None, :]
    out_ref[dim + 1 :, :] = 2.0 * bits_ref[...].astype(jnp.float32) - 1.0


def blocks_of(refs):
    return [(ref, k) for ref in refs for k in range(ref.shape[0])]


def product(both, high, low):
    count = both.shape[0] // 2
    main = jnp.dot(both, high, preferred_element_type=jnp.float32)
    return (main[:count] + main[count:]) + jnp.dot(both[:count], low, preferred_element_type=jnp.float32)


def build_kernel(pieces, dim, *refs):
    ins, refs = refs[:pieces], refs[pieces:]
    signal_ref, noise_ref, high_ref, low_ref, vec_ref, image_ref, feature_ref, both_ref = refs
    count, width = image_ref.shape
    blocks = blocks_of(ins)
    own = features(ins[0][0, :dim, :], True)

    for at, (ref, k) in enumerate(blocks):
        rows = pl.ds(at * width, width)
        feature_ref[rows, :] = features(ref[k, :dim, :], False).T
        vector = ref[k, dim:, :]
        vec_ref[:, columns(at, width)] = vector
        both_ref[at] = jnp.concatenate(split_two(vector), axis=0)

    def tile_of(at):
        rows = pl.ds(pl.multiple_of(at * width, width), width)
        dist = jnp.dot(feature_ref[rows, :], own, preferred_element_type=jnp.float32)
        dist = jnp.maximum(dist, 1e-30)
        radius = dist * lax.rsqrt(dist)
        tile = ((1.0 + dist * (1.0 / 3.0)) + radius) * jnp.exp2(radius * (-LOG2_E))
        high, low = split_two(tile)
        high_ref[rows, :] = high
        low_ref[rows, :] = low
        return high, low

    def one(group, total):
        for k in range(UNROLL):
            at = group * UNROLL + k
            total = total + product(both_ref[at], *tile_of(at))
        return total

    total = lax.fori_loop(0, len(blocks) // UNROLL, one, jnp.zeros((count, width), jnp.float32))
    image_ref[...] = signal_ref[0] * total + noise_ref[0] * vec_ref[:, :width]


def summed(total):
    return jnp.sum(total, axis=1, keepdims=True)


def step_kernel(pieces, first, last, *refs):
    ins, refs = refs[:pieces], list(refs[pieces:])
    signal_ref, noise_ref, high_ref, low_ref, res_ref = refs[:5]
    refs = refs[5:]
    if first:
        dir_ref = res_ref
    else:
        dir_ref, norm_ref, sol_ref = refs[:3]
        refs = refs[3:]
    if last:
        new_res_ref, new_dir_ref, new_norm_ref, new_sol_ref, image_ref, share_ref, both_ref = refs
    else:
        new_res_ref, new_dir_ref, new_norm_ref, new_sol_ref, image_ref, both_ref = refs
    count, width = image_ref.shape
    blocks = blocks_of(ins)
    zero = jnp.zeros((count, width), jnp.float32)

    along, square = zero, zero
    for at, (ref, k) in enumerate(blocks):
        direction = dir_ref[:, columns(at, width)]
        along = along + direction * ref[k]
        if first:
            square = square + direction * direction
    norm = summed(square) if first else norm_ref[...]
    alpha = norm / summed(along)
    so_far = alpha * dir_ref[:, :width]
    new_sol_ref[...] = so_far if first else sol_ref[...] + so_far

    square = zero
    for at, (ref, k) in enumerate(blocks):
        here = columns(at, width)
        residual = res_ref[:, here] - alpha * ref[k]
        square = square + residual * residual
    new_norm = summed(square)
    new_norm_ref[...] = new_norm
    beta = new_norm / norm

    for at, (ref, k) in enumerate(blocks):
        here = columns(at, width)
        residual = res_ref[:, here] - alpha * ref[k]
        direction = residual + beta * dir_ref[:, here]
        if not last:
            new_res_ref[:, here] = residual
            new_dir_ref[:, here] = direction
        elif at == 0:
            new_dir_ref[...] = direction
            new_res_ref[...] = residual
        both_ref[:, here] = jnp.concatenate(split_two(direction), axis=0)
    total = product(both_ref[...], high_ref[...], low_ref[...])
    image = signal_ref[0] * total + noise_ref[0] * new_dir_ref[:, :width]
    image_ref[...] = image
    if last:
        share = jnp.broadcast_to(summed(new_dir_ref[...] * image), (count, 128))
        share_ref[...] = share.T[: share_ref.shape[0]]


def last_kernel(shares_ref, norm_ref, sol_ref, dir_ref, res_ref, image_ref, out_ref, out_res_ref):
    count = norm_ref.shape[0]
    total = jnp.sum(shares_ref[...], axis=0, keepdims=True)
    total = jnp.broadcast_to(total, (128, count)).T[:, :1]
    alpha = norm_ref[...] / total
    out_ref[...] = sol_ref[...] + alpha * dir_ref[...]
    out_res_ref[...] = res_ref[...] - alpha * image_ref[...]


UNROLL = 4
VMEM = pl.BlockSpec(memory_space=pltpu.VMEM)
SMEM = pl.BlockSpec(memory_space=pltpu.SMEM)


def nbytes(*shapes):
    return sum(math.prod(s.shape) * s.dtype.itemsize for s in shapes)


def call(kernel, ins, specs, outs, scratch=(), flops=1000):
    room = nbytes(*ins, *outs) + sum(nbytes(jax.ShapeDtypeStruct(s.shape, s.dtype)) for s in scratch)
    return pl.pallas_call(
        kernel,
        out_shape=tuple(outs),
        in_specs=specs,
        out_specs=(VMEM,) * len(outs),
        scratch_shapes=list(scratch),
        compiler_params=pltpu.CompilerParams(vmem_limit_bytes=min(room * 5 // 4 + (6 << 20), 62 << 20)),
        cost_estimate=pl.CostEstimate(flops=flops, bytes_accessed=room, transcendentals=0),
    )(*ins)


def body(mesh_shape, points, lengthscale, signal, noise, targets, probe_bits):
    devices = mesh_shape[0] * mesh_shape[1]
    dim, width = points.shape
    count = probe_bits.shape[0] + 1

    def f32(*shape):
        return jax.ShapeDtypeStruct(shape, jnp.float32)

    every = devices * width
    matrix = jax.ShapeDtypeStruct((every, width), jnp.bfloat16)
    flops = 2 * every * width

    (payload,) = call(
        payload_kernel,
        (points, lengthscale, targets, probe_bits),
        [VMEM, SMEM, VMEM, VMEM],
        [f32(dim + count, width)],
    )
    pieces = gather(payload, mesh_shape)
    scales, scale_specs = (signal, noise), [SMEM] * 2
    high, low, residual, image = call(
        functools.partial(build_kernel, len(pieces), dim),
        (*pieces, *scales),
        [VMEM] * len(pieces) + scale_specs,
        [matrix, matrix, f32(count, every), f32(count, width)],
        [
            pltpu.VMEM((every, FEATURES), jnp.bfloat16),
            pltpu.VMEM((devices, 2 * count, width), jnp.bfloat16),
        ],
        flops * 300,
    )
    state = (residual,)
    for number in range(ITERS - 1):
        last = number == ITERS - 2
        pieces = gather(image, mesh_shape)
        held = f32(count, width if last else every)
        outs = call(
            functools.partial(step_kernel, len(pieces), number == 0, last),
            (*pieces, *scales, high, low, *state),
            [VMEM] * len(pieces) + scale_specs + [VMEM] * (2 + len(state)),
            [held, held, f32(count, 1), f32(count, width), f32(count, width)]
            + ([f32(devices, count)] if last else []),
            [pltpu.VMEM((2 * count, every), jnp.bfloat16)],
            flops * 100,
        )
        state, image = outs[:4], outs[4]
    residual, direction, norm, so_far = state
    shares = lax.all_to_all(outs[5], AXES, 0, 0, tiled=True)
    return call(
        last_kernel,
        (shares, norm, so_far, direction, residual, image),
        [VMEM] * 6,
        [f32(count, width)] * 2,
    )


def solution(mesh):
    shape = (mesh.shape["row"], mesh.shape["col"])
    return jax.shard_map(
        functools.partial(body, shape),
        mesh=mesh,
        in_specs=(
            P(None, AXES),
            P(),
            P(),
            P(),
            P(AXES),
            P(None, AXES),
        ),
        out_specs=(P(None, AXES), P(None, AXES)),
        check_vma=False,
    )
```
